32 devices in a mesh: section: 4 (over y, x), dp: 8 (over z, core).
Axes of the slice: x: 2, y: 2, z: 4, core: 2. Of those that a mesh axis runs over, the one named last changes fastest.
Arguments:
- block_inputs: bfloat16 [4, 4, 512, 2048], P('section', None, 'dp'), may hold values from -6 to 6
- mixed_inputs: bfloat16 [4, 4, 512, 2048], P('section', None, 'dp'), may hold values from -6 to 6
- token_ids: int32 [4, 512], P(None, 'dp'), may hold values from 0 to 2047
- target_ids: int32 [4, 512], P(None, 'dp'), may hold values from 0 to 2047
- final_gain: float32 [2048], replicated, may hold values from 0.5 to 1.5
- out_weight: bfloat16 [4, 2048, 2048], P('section'), may hold values from -0.0625 to 0.0625
- head_weight: bfloat16 [2048, 2048], P('section'), may hold values from -0.375 to 0.375
- out_master: float32 [4, 2048, 2048], P('section', 'dp'), may hold values from -0.125 to 0.125
- out_first: float32 [4, 2048, 2048], P('section', 'dp'), may hold values from -1.25 to 1.25
- out_second: float32 [4, 2048, 2048], P('section', 'dp'), may hold values from 1 to 20
- head_master: float32 [2048, 2048], P(('section', 'dp')), may hold values from -0.125 to 0.125
- head_first: float32 [2048, 2048], P(('section', 'dp')), may hold values from -0.75 to 0.75
- head_second: float32 [2048, 2048], P(('section', 'dp')), may hold values from 0.3 to 6
- embed_master: float32 [2048, 2048], P(('section', 'dp')), may hold values from -0.125 to 0.125
- embed_first: float32 [2048, 2048], P(('section', 'dp')), may hold values from -0.0625 to 0.0625
- embed_second: float32 [2048, 2048], P(('section', 'dp')), may hold values from 0.0024414062 to 0.048828125
Outputs:
- out_master_next: float32 [4, 2048, 2048], P('section', 'dp')
- out_first_next: float32 [4, 2048, 2048], P('section', 'dp')
- out_second_next: float32 [4, 2048, 2048], P('section', 'dp')
- head_master_next: float32 [2048, 2048], P(('section', 'dp'))
- head_first_next: float32 [2048, 2048], P(('section', 'dp'))
- head_second_next: float32 [2048, 2048], P(('section', 'dp'))
- embed_master_next: float32 [2048, 2048], P(('section', 'dp'))
- embed_first_next: float32 [2048, 2048], P(('section', 'dp'))
- embed_second_next: float32 [2048, 2048], P(('section', 'dp'))
The draws below stay inside these ranges and needn't reach their ends.
Inputs may be any that keep to these rules, and one draw needn't show every extreme that they name: `token_ids`: every token id lies in 0 to 2047. `target_ids`: every target id lies in 0 to 2047.
All inputs are finite; a program needn't handle non-finite values.
Results may differ from the reference program's by a relative error of at most 0.00155.
Values may be sent and summed in bfloat16 or wider, within the bound.
A program may use at most 128 MiB of HBM per device.

```python
import math
import jax
import jax.numpy as jnp
import numpy as np
from jax import lax

D = 2048
VOCAB = 2048
MICRO = 4
TOKENS_MB = 512
N_SECTION = 4


def with_ends(entries, key, least, largest):
    longest = entries.shape.index(max(entries.shape))
    spots = []
    for shift in (0, 1):
        where = [jax.random.randint(jax.random.fold_in(key, axis), (), 0, length) for axis, length in enumerate(entries.shape)]
        where[longest] = (where[longest] + shift) % entries.shape[longest]
        spots.append(tuple(where))
    return entries.at[spots[0]].set(least).at[spots[1]].set(largest)


def level_of(key, shape, shards, least, top_value):
    level = 1.0
    for position, shards_of in shards:
        steps = jax.random.uniform(jax.random.fold_in(jax.random.fold_in(key, 6), position), (shards_of,), jnp.float32, least / len(shards), top_value / len(shards))
        level = level * jnp.repeat(jnp.exp(steps), shape[position] // shards_of).reshape((-1,) + (1,) * (len(shape) - 1 - position))
    return level


def rank_table(amount, skew):
    portions = [(1 << 20) // math.isqrt(grade ** skew) + 1 for grade in range(1, amount + 1)]
    deviation = 1 + sum(portions) // (1 << 30)
    return np.cumsum(np.array([max(1, weight // deviation) for weight in portions]))


def ranked_ids(own_key, shape, number_of, slope):
    grid = rank_table(number_of, slope)
    ticket = jax.random.randint(jax.random.fold_in(own_key, 1), shape, 0, int(grid[number_of - 1]))
    rank = jnp.searchsorted(jnp.asarray(grid, jnp.int32), ticket, side="right")
    return jax.random.permutation(jax.random.fold_in(own_key, 2), number_of)[rank].astype(jnp.int32)


def centred(stream_key, shape, spread, bound, pieces=(), dtype=jnp.bfloat16):
    result = spread * jax.random.normal(stream_key, shape, jnp.float32)
    if pieces:
        result = result * level_of(stream_key, shape, pieces, -0.22, 0.18)
    return jnp.clip(result, -bound, bound).astype(dtype)


def setup_inputs(seed: int = 0) -> dict:
    arg_keys = jax.random.split(jax.random.key(seed), 17)
    return {
        "block_inputs": centred(arg_keys[0], (N_SECTION, MICRO, TOKENS_MB, D), 1.0, 6.0, ((0, 4), (2, 8))),
        "mixed_inputs": centred(arg_keys[1], (N_SECTION, MICRO, TOKENS_MB, D), 1.0, 6.0, ((0, 4), (2, 8))),
        "token_ids": with_ends(ranked_ids(arg_keys[2], (MICRO, TOKENS_MB), VOCAB, 2), jax.random.fold_in(arg_keys[2], 3), 0, VOCAB - 1).astype(jnp.int32),
        "target_ids": with_ends(ranked_ids(arg_keys[3], (MICRO, TOKENS_MB), VOCAB, 2), jax.random.fold_in(arg_keys[3], 3), 0, VOCAB - 1).astype(jnp.int32),
        "final_gain": jnp.clip(1.0 + 0.1 * jax.random.normal(arg_keys[4], (D,), jnp.float32), 0.5, 1.5),
        "out_weight": centred(arg_keys[5], (N_SECTION, D, D), (D * N_SECTION) ** -0.5, 0.0625, ((0, 4),)),
        "head_weight": centred(arg_keys[6], (VOCAB, D), (3 * D ** -0.5), 0.375, ((0, 4),)),
        "out_master": centred(arg_keys[7], (N_SECTION, D, D), D ** -0.5, 0.125, ((0, 4), (1, 8)), jnp.float32),
        "out_first": centred(arg_keys[8], (N_SECTION, D, D), (0.2 * (MICRO * TOKENS_MB) ** 0.5 * D ** -0.5), 1.25, ((0, 4), (1, 8)), jnp.float32),
        "out_second": jnp.clip(jnp.exp(math.log(20.0) - 2.9957323 * jax.random.uniform(arg_keys[9], (N_SECTION, D, D), jnp.float32) ** level_of(arg_keys[9], (N_SECTION, D, D), ((0, 4), (1, 8)), -0.2, 0.2)), 1.0, 20.0),
        "head_master": centred(arg_keys[10], (VOCAB, D), D ** -0.5, 0.125, ((0, 32),), jnp.float32),
        "head_first": centred(arg_keys[11], (VOCAB, D), (0.12 * (MICRO * TOKENS_MB) ** 0.5 * VOCAB ** -0.5), 0.75, ((0, 32),), jnp.float32),
        "head_second": jnp.clip(jnp.exp(math.log(6.0) - 2.9957322 * jax.random.uniform(arg_keys[12], (VOCAB, D), jnp.float32) ** level_of(arg_keys[12], (VOCAB, D), ((0, 32),), -0.2, 0.2)), 0.3, 6.0),
        "embed_master": centred(arg_keys[13], (VOCAB, D), D ** -0.5, 0.125, ((0, 32),), jnp.float32),
        "embed_first": centred(arg_keys[14], (VOCAB, D), (0.5 * (MICRO * TOKENS_MB) ** 0.5 * (VOCAB * D) ** -0.5), 0.0625, ((0, 32),), jnp.float32),
        "embed_second": jnp.clip(jnp.exp(math.log(0.048828125) - 2.9957323 * jax.random.uniform(arg_keys[15], (VOCAB, D), jnp.float32) ** level_of(arg_keys[15], (VOCAB, D), ((0, 32),), -0.2, 0.2)), 0.0024414062, 0.048828125),
    }


norm_eps = 1e-05
beta_first = 0.9
beta_second = 0.95
adam_eps = 1e-05
learning_rate = 0.0003
decay_rate = 0.1

def times_transposed(former, latter):
    return lax.dot_general(former, latter, (((1,), (1,)), ((), ())), preferred_element_type=jnp.float32)

def transposed_times(former, latter):
    return lax.dot_general(former, latter, (((0,), (0,)), ((), ())), preferred_element_type=jnp.float32)

def plain_times(former, latter):
    return jnp.dot(former, latter, preferred_element_type=jnp.float32)

def normalize(values, gain):
    inverse = lax.rsqrt(lax.optimization_barrier(jnp.mean(values * values, axis=-1, keepdims=True)) + norm_eps)
    return (inverse, values * inverse * gain)

def norm_backward(values, inverse, scaled_cotangent):
    unit = values * inverse
    return inverse * (scaled_cotangent - unit * lax.optimization_barrier(jnp.mean(scaled_cotangent * unit, axis=-1, keepdims=True)))

def adam_update(master, first, second, gradient):
    first_next = beta_first * first + (1.0 - beta_first) * gradient
    second_next = beta_second * second + (1.0 - beta_second) * gradient * gradient
    master_next = master - learning_rate * (first_next / (jnp.sqrt(second_next) + adam_eps) + decay_rate * master)
    return (master_next, first_next, second_next)

def reference(block_inputs, mixed_inputs, token_ids, target_ids, final_gain, out_weight, head_weight, out_master, out_first, out_second, head_master, head_first, head_second, embed_master, embed_first, embed_second):
    last = N_SECTION - 1
    count = MICRO * TOKENS_MB
    wide = block_inputs[last].reshape(count, D).astype(jnp.float32)
    final = wide + times_transposed(mixed_inputs[last].reshape(count, D), out_weight[last])
    final_inverse, final_scaled = normalize(final, final_gain)
    last_hidden = final_scaled.astype(jnp.bfloat16)
    logits = times_transposed(last_hidden, head_weight)
    predicted = jax.nn.softmax(logits, axis=-1)
    columns = lax.broadcasted_iota(jnp.int32, (1, VOCAB), 1)
    hits = (target_ids.reshape(-1)[:, None] == columns).astype(jnp.float32)
    logit_cotangent = (predicted - hits).astype(jnp.bfloat16)
    head_gradient = transposed_times(logit_cotangent, last_hidden)
    hidden_cotangent = plain_times(logit_cotangent, head_weight)
    cotangent = norm_backward(final, final_inverse, hidden_cotangent * final_gain).astype(jnp.bfloat16)
    parts = []
    for section in range(N_SECTION):
        parts.append(transposed_times(cotangent, mixed_inputs[section].reshape(count, D)))
    out_gradient = jnp.stack(parts)
    embed_gradient = jax.ops.segment_sum(cotangent.astype(jnp.float32), token_ids.reshape(-1), num_segments=VOCAB)
    out_out = adam_update(out_master, out_first, out_second, out_gradient)
    head_out = adam_update(head_master, head_first, head_second, head_gradient)
    embed_out = adam_update(embed_master, embed_first, embed_second, embed_gradient)
    return (out_out[0], out_out[1], out_out[2], head_out[0], head_out[1], head_out[2], embed_out[0], embed_out[1], embed_out[2])
```

```python
import functools
import jax
import jax.numpy as jnp
from jax import lax
from jax.experimental import pallas as pl
from jax.experimental.pallas import tpu as pltpu
from jax.sharding import PartitionSpec as P

norm_eps = 1e-05
beta_first = 0.9
beta_second = 0.95
adam_eps = 1e-05
learning_rate = 0.0003
decay_rate = 0.1

MESH = pl.DeviceIdType.MESH


def times_transposed(former, latter):
    return lax.dot_general(
        former, latter, (((1,), (1,)), ((), ())), preferred_element_type=jnp.float32
    )


def transposed_times(former, latter):
    return lax.dot_general(
        former, latter, (((0,), (0,)), ((), ())), preferred_element_type=jnp.float32
    )


def plain_times(former, latter):
    return jnp.dot(former, latter, preferred_element_type=jnp.float32)


def adam_update(master, first, second, gradient):
    first_next = beta_first * first + (1.0 - beta_first) * gradient
    second_next = beta_second * second + (1.0 - beta_second) * gradient * gradient
    master_next = master - learning_rate * (
        first_next / (jnp.sqrt(second_next) + adam_eps) + decay_rate * master
    )
    return (master_next, first_next, second_next)


def greet(axis, size, me):
    barrier = pltpu.get_barrier_semaphore()
    for step in range(1, size):
        partner = lax.rem(me + step, size)
        pl.semaphore_signal(barrier, inc=1, device_id={axis: partner}, device_id_type=MESH)
    pl.semaphore_wait(barrier, size - 1)


def exchange_kernel(axis, size, modes, *refs):
    count = len(modes)
    ins, outs = refs[:count], refs[count : 2 * count]
    send_sem, recv_sem = refs[2 * count :]
    me = lax.axis_index(axis)
    greet(axis, size, me)
    copies = []
    for step in range(1, size):
        partner = lax.rem(me + step, size)
        for k, mode in enumerate(modes):
            copy = pltpu.make_async_remote_copy(
                src_ref=ins[k] if mode == "share" else ins[k].at[partner],
                dst_ref=outs[k].at[step - 1 if mode == "others" else me],
                send_sem=send_sem.at[k, step - 1],
                recv_sem=recv_sem.at[k, step - 1],
                device_id={axis: partner},
                device_id_type=MESH,
            )
            copy.start()
            copies.append(copy)
    for k, mode in enumerate(modes):
        if mode != "others":
            outs[k][me] = ins[k][me] if mode == "swap" else ins[k][...]
    for copy in copies:
        copy.wait()


def exchange(arrays, modes, axis, collective_id):
    size = lax.axis_size(axis)
    lead = {"swap": (size,), "share": (size,), "others": (size - 1,)}
    shapes = [
        jax.ShapeDtypeStruct(lead[mode] + (a.shape if mode == "share" else a.shape[1:]), a.dtype)
        for a, mode in zip(arrays, modes)
    ]
    return pl.pallas_call(
        functools.partial(exchange_kernel, axis, size, tuple(modes)),
        out_shape=shapes,
        in_specs=[pl.BlockSpec(memory_space=pltpu.VMEM)] * len(arrays),
        out_specs=[pl.BlockSpec(memory_space=pltpu.VMEM)] * len(arrays),
        scratch_shapes=[
            pltpu.SemaphoreType.DMA((len(arrays), size - 1)),
            pltpu.SemaphoreType.DMA((len(arrays), size - 1)),
        ],
        compiler_params=pltpu.CompilerParams(collective_id=collective_id, has_side_effects=True),
    )(*arrays)


def spread_kernel(axis, size, chunks, in_ref, out_ref, send_sem, recv_sem):
    me = lax.axis_index(axis)
    place = me
    shift = me // 2
    while_size = size
    while while_size > 2:
        place = place ^ shift
        shift = shift // 2
        while_size //= 2

    def device_at(position):
        position = lax.rem(position + size, size)
        return position ^ (position // 2)

    source_place = 0
    for candidate in range(size):
        if candidate ^ (candidate // 2) == size - 1:
            source_place = candidate
    distance = lax.rem(place - source_place + size, size)
    forward, behind = device_at(place + 1), device_at(place - 1)
    barrier = pltpu.get_barrier_semaphore()
    for partner in (forward, behind):
        pl.semaphore_signal(barrier, inc=1, device_id={axis: partner}, device_id_type=MESH)
    pl.semaphore_wait(barrier, 2)
    piece = in_ref.shape[0] // (2 * chunks)

    def copy_of(way, chunk, ref):
        rows = pl.ds((way * chunks + chunk) * piece, piece)
        return pltpu.make_async_remote_copy(
            src_ref=ref.at[rows],
            dst_ref=out_ref.at[rows],
            send_sem=send_sem.at[way, chunk],
            recv_sem=recv_sem.at[way, chunk],
            device_id={axis: forward if way == 0 else behind},
            device_id_type=MESH,
        )

    @pl.when(distance == 0)
    def _():
        for chunk in range(chunks):
            for way in range(2):
                copy_of(way, chunk, in_ref).start()
        out_ref[...] = in_ref[...]
        for chunk in range(chunks):
            for way in range(2):
                copy_of(way, chunk, in_ref).wait_send()

    @pl.when(distance > 0)
    def _():
        for chunk in range(chunks):
            for way in range(2):
                hops = distance if way == 0 else size - distance
                copy_of(way, chunk, out_ref).wait_recv()

                @pl.when(hops < size - 1)
                def _():
                    copy_of(way, chunk, out_ref).start()

        for chunk in range(chunks):
            for way in range(2):
                hops = distance if way == 0 else size - distance

                @pl.when(hops < size - 1)
                def _():
                    copy_of(way, chunk, out_ref).wait_send()


def spread(block, axis, collective_id, chunks=8):
    size = lax.axis_size(axis)
    return pl.pallas_call(
        functools.partial(spread_kernel, axis, size, chunks),
        out_shape=jax.ShapeDtypeStruct(block.shape, block.dtype),
        in_specs=[pl.BlockSpec(memory_space=pltpu.VMEM)],
        out_specs=pl.BlockSpec(memory_space=pltpu.VMEM),
        scratch_shapes=[
            pltpu.SemaphoreType.DMA((2, chunks)),
            pltpu.SemaphoreType.DMA((2, chunks)),
        ],
        compiler_params=pltpu.CompilerParams(collective_id=collective_id, has_side_effects=True),
        name="spread",
    )(block)


def local(
    block_inputs,
    mixed_inputs,
    token_ids,
    target_ids,
    final_gain,
    out_weight,
    head_weight,
    out_master,
    out_first,
    out_second,
    head_master,
    head_first,
    head_second,
    embed_master,
    embed_first,
    embed_second,
):
    sections = lax.axis_size("section")
    replicas = lax.axis_size("dp")
    section = lax.axis_index("section")
    last = sections - 1
    batches, rows, width = mixed_inputs[0].shape
    tokens = batches * rows
    share = tokens // sections
    columns_own = width // replicas
    flat_mixed = mixed_inputs[0].reshape(tokens, width)
    all_mixed = lax.all_gather(flat_mixed, "dp", tiled=True)
    wide = block_inputs[0].reshape(tokens, width).astype(jnp.float32)
    slice_rows = head_weight.shape[0]
    vocabulary_start = section * slice_rows
    columns = vocabulary_start + lax.broadcasted_iota(jnp.int32, (1, slice_rows), 1)
    final = wide + times_transposed(flat_mixed, out_weight[0])
    final_inverse = lax.rsqrt(jnp.mean(final * final, axis=-1, keepdims=True) + norm_eps)
    own_hidden = (final * final_inverse * final_gain).astype(jnp.bfloat16)
    hidden = spread(own_hidden, "section", 0)
    logits = times_transposed(hidden, head_weight)
    local_top = jnp.max(logits, axis=1)
    local_weights = jnp.exp(logits - local_top[:, None])
    (stats,) = exchange(
        [jnp.stack([local_top, jnp.sum(local_weights, axis=1), final_inverse[:, 0]])],
        ["share"],
        "section",
        1,
    )
    row_top = jnp.max(stats[:, 0], axis=0)
    row_total = jnp.sum(stats[:, 1] * jnp.exp(stats[:, 0] - row_top), axis=0)
    predicted = local_weights * (jnp.exp(local_top - row_top) / row_total)[:, None]
    target_flat = target_ids.reshape(-1)
    logit_cotangent = jnp.where(target_flat[:, None] == columns, predicted - 1.0, predicted).astype(
        jnp.bfloat16
    )
    hidden_part = plain_times(logit_cotangent, head_weight).reshape(sections, share, width)
    (hidden_parts,) = exchange(
        [hidden_part], ["others"], "section", 2
    )
    hidden_cotangent = (
        lax.dynamic_index_in_dim(hidden_part, section, 0, False)
        + jnp.sum(hidden_parts, axis=0)
    )
    inverse = lax.dynamic_slice_in_dim(stats[last, 2], section * share, share)[:, None]
    unit = lax.dynamic_slice_in_dim(hidden, section * share, share).astype(jnp.float32) / final_gain
    scaled = hidden_cotangent * final_gain
    cotangent = (
        inverse * (scaled - unit * jnp.mean(scaled * unit, axis=-1, keepdims=True))
    ).astype(jnp.bfloat16)
    head_part = transposed_times(logit_cotangent, hidden)
    head_gradient = lax.psum_scatter(
        head_part, "dp", scatter_dimension=0, tiled=True
    )
    pieces = cotangent.reshape(share, replicas, columns_own).transpose(1, 0, 2)
    own_columns, all_tokens = exchange(
        [pieces, token_ids.reshape(1, tokens)], ["swap", "share"], "dp", 3
    )
    (all_columns,) = exchange([own_columns], ["share"], "section", 4)
    cotangent_columns = all_columns.transpose(1, 0, 2, 3).reshape(replicas * tokens, columns_own)
    marks = (all_tokens.reshape(-1, 1) == columns).astype(jnp.bfloat16)
    embed_columns = transposed_times(marks, cotangent_columns)
    (embed_parts,) = exchange(
        [embed_columns.reshape(replicas, slice_rows // replicas, columns_own)], ["swap"], "dp", 5
    )
    embed_gradient = (
        embed_parts.astype(jnp.float32).transpose(1, 0, 2).reshape(slice_rows // replicas, width)
    )
    out_gradient = transposed_times(cotangent_columns, all_mixed)
    out_out = adam_update(out_master, out_first, out_second, out_gradient.reshape(out_master.shape))
    head_out = adam_update(head_master, head_first, head_second, head_gradient)
    embed_out = adam_update(embed_master, embed_first, embed_second, embed_gradient)
    return out_out + head_out + embed_out


def solution(mesh):
    return jax.shard_map(
        local,
        mesh=mesh,
        in_specs=(
            P("section", None, "dp", None),
            P("section", None, "dp", None),
            P(None, "dp"),
            P(None, "dp"),
            P(),
            P("section", None, None),
            P("section", None),
            P("section", "dp", None),
            P("section", "dp", None),
            P("section", "dp", None),
            P(("section", "dp"), None),
            P(("section", "dp"), None),
            P(("section", "dp"), None),
            P(("section", "dp"), None),
            P(("section", "dp"), None),
            P(("section", "dp"), None),
        ),
        out_specs=(
            P("section", "dp", None),
            P("section", "dp", None),
            P("section", "dp", None),
            P(("section", "dp"), None),
            P(("section", "dp"), None),
            P(("section", "dp"), None),
            P(("section", "dp"), None),
            P(("section", "dp"), None),
            P(("section", "dp"), None),
        ),
        check_vma=False,
    )
```

```python
import functools
import jax
import jax.numpy as jnp
from jax import lax
from jax.experimental import pallas as pl
from jax.experimental.pallas import tpu as pltpu
from jax.sharding import PartitionSpec as P

norm_eps = 1e-05
beta_first = 0.9
beta_second = 0.95
adam_eps = 1e-05
learning_rate = 0.0003
decay_rate = 0.1

MESH = pl.DeviceIdType.MESH


def times_transposed(former, latter):
    return lax.dot_general(
        former, latter, (((1,), (1,)), ((), ())), preferred_element_type=jnp.float32
    )


def transposed_times(former, latter):
    return lax.dot_general(
        former, latter, (((0,), (0,)), ((), ())), preferred_element_type=jnp.float32
    )


def plain_times(former, latter):
    return jnp.dot(former, latter, preferred_element_type=jnp.float32)


def adam_update(master, first, second, gradient):
    first_next = beta_first * first + (1.0 - beta_first) * gradient
    second_next = beta_second * second + (1.0 - beta_second) * gradient * gradient
    master_next = master - learning_rate * (
        first_next / (jnp.sqrt(second_next) + adam_eps) + decay_rate * master
    )
    return (master_next, first_next, second_next)


def greet(axis, size, me):
    barrier = pltpu.get_barrier_semaphore()
    for step in range(1, size):
        partner = lax.rem(me + step, size)
        pl.semaphore_signal(barrier, inc=1, device_id={axis: partner}, device_id_type=MESH)
    pl.semaphore_wait(barrier, size - 1)


def exchange_kernel(axis, size, modes, *refs):
    count = len(modes)
    ins, outs = refs[:count], refs[count : 2 * count]
    send_sem, recv_sem = refs[2 * count :]
    me = lax.axis_index(axis)
    greet(axis, size, me)
    copies = []
    for step in range(1, size):
        partner = lax.rem(me + step, size)
        for k, mode in enumerate(modes):
            copy = pltpu.make_async_remote_copy(
                src_ref=ins[k] if mode == "share" else ins[k].at[partner],
                dst_ref=outs[k].at[step - 1 if mode == "others" else me],
                send_sem=send_sem.at[k, step - 1],
                recv_sem=recv_sem.at[k, step - 1],
                device_id={axis: partner},
                device_id_type=MESH,
            )
            copy.start()
            copies.append(copy)
    for k, mode in enumerate(modes):
        if mode != "others":
            outs[k][me] = ins[k][me] if mode == "swap" else ins[k][...]
    for copy in copies:
        copy.wait()


def exchange(arrays, modes, axis, collective_id):
    size = lax.axis_size(axis)
    lead = {"swap": (size,), "share": (size,), "others": (size - 1,)}
    shapes = [
        jax.ShapeDtypeStruct(lead[mode] + (a.shape if mode == "share" else a.shape[1:]), a.dtype)
        for a, mode in zip(arrays, modes)
    ]
    return pl.pallas_call(
        functools.partial(exchange_kernel, axis, size, tuple(modes)),
        out_shape=shapes,
        in_specs=[pl.BlockSpec(memory_space=pltpu.VMEM)] * len(arrays),
        out_specs=[pl.BlockSpec(memory_space=pltpu.VMEM)] * len(arrays),
        scratch_shapes=[
            pltpu.SemaphoreType.DMA((len(arrays), size - 1)),
            pltpu.SemaphoreType.DMA((len(arrays), size - 1)),
        ],
        compiler_params=pltpu.CompilerParams(collective_id=collective_id, has_side_effects=True),
    )(*arrays)


def spread_kernel(axis, size, in_ref, out_ref, send_sem, recv_sem):
    me = lax.axis_index(axis)
    last = size - 1
    second = last // 2
    piece = in_ref.shape[0] // size
    greet(axis, size, me)

    def copy_of(part, target, ref):
        rows = pl.ds(part * piece, piece)
        return pltpu.make_async_remote_copy(
            src_ref=ref.at[rows],
            dst_ref=out_ref.at[rows],
            send_sem=send_sem.at[part, target],
            recv_sem=recv_sem.at[part],
            device_id={axis: target},
            device_id_type=MESH,
        )

    def relayed(device):
        return [device, last] if device == second else [device]

    @pl.when(me == last)
    def _():
        copies = [copy_of(part, k, in_ref) for k in range(last) for part in relayed(k)]
        for copy in copies:
            copy.start()
        out_ref[...] = in_ref[...]
        for copy in copies:
            copy.wait_send()

    for device in range(last):

        @pl.when(me == device)
        def _():
            others = [k for k in range(last) if k != device]
            copies = []
            for part in relayed(device):
                copy_of(part, others[0], out_ref).wait_recv()
                for k in others:
                    copies.append(copy_of(part, k, out_ref))
                    copies[-1].start()
            for part in range(size):
                if part not in relayed(device):
                    copy_of(part, others[0], out_ref).wait_recv()
            for copy in copies:
                copy.wait_send()


def spread(block, axis, collective_id):
    size = lax.axis_size(axis)
    return pl.pallas_call(
        functools.partial(spread_kernel, axis, size),
        out_shape=jax.ShapeDtypeStruct(block.shape, block.dtype),
        in_specs=[pl.BlockSpec(memory_space=pltpu.VMEM)],
        out_specs=pl.BlockSpec(memory_space=pltpu.VMEM),
        scratch_shapes=[
            pltpu.SemaphoreType.DMA((size, size)),
            pltpu.SemaphoreType.DMA((size,)),
        ],
        compiler_params=pltpu.CompilerParams(collective_id=collective_id, has_side_effects=True),
        name="spread",
    )(block)


def local(
    block_inputs,
    mixed_inputs,
    token_ids,
    target_ids,
    final_gain,
    out_weight,
    head_weight,
    out_master,
    out_first,
    out_second,
    head_master,
    head_first,
    head_second,
    embed_master,
    embed_first,
    embed_second,
):
    sections = lax.axis_size("section")
    replicas = lax.axis_size("dp")
    section = lax.axis_index("section")
    last = sections - 1
    batches, rows, width = mixed_inputs[0].shape
    tokens = batches * rows
    share = tokens // sections
    columns_own = width // replicas
    flat_mixed = mixed_inputs[0].reshape(tokens, width)
    all_mixed = lax.all_gather(flat_mixed, "dp", tiled=True)
    wide = block_inputs[0].reshape(tokens, width).astype(jnp.float32)
    slice_rows = head_weight.shape[0]
    vocabulary_start = section * slice_rows
    columns = vocabulary_start + lax.broadcasted_iota(jnp.int32, (1, slice_rows), 1)
    final = wide + times_transposed(flat_mixed, out_weight[0])
    final_inverse = lax.rsqrt(jnp.mean(final * final, axis=-1, keepdims=True) + norm_eps)
    own_hidden = (final * final_inverse * final_gain).astype(jnp.bfloat16)
    hidden = spread(own_hidden, "section", 0)
    logits = times_transposed(hidden, head_weight)
    local_top = jnp.max(logits, axis=1)
    local_weights = jnp.exp(logits - local_top[:, None])
    (stats,) = exchange(
        [jnp.stack([local_top, jnp.sum(local_weights, axis=1), final_inverse[:, 0]])],
        ["share"],
        "section",
        1,
    )
    row_top = jnp.max(stats[:, 0], axis=0)
    row_total = jnp.sum(stats[:, 1] * jnp.exp(stats[:, 0] - row_top), axis=0)
    predicted = local_weights * (jnp.exp(local_top - row_top) / row_total)[:, None]
    target_flat = target_ids.reshape(-1)
    logit_cotangent = jnp.where(target_flat[:, None] == columns, predicted - 1.0, predicted).astype(
        jnp.bfloat16
    )
    hidden_part = plain_times(logit_cotangent, head_weight).reshape(sections, share, width)
    (hidden_parts,) = exchange(
        [hidden_part], ["others"], "section", 2
    )
    hidden_cotangent = (
        lax.dynamic_index_in_dim(hidden_part, section, 0, False)
        + jnp.sum(hidden_parts, axis=0)
    )
    inverse = lax.dynamic_slice_in_dim(stats[last, 2], section * share, share)[:, None]
    unit = lax.dynamic_slice_in_dim(hidden, section * share, share).astype(jnp.float32) / final_gain
    scaled = hidden_cotangent * final_gain
    cotangent = (
        inverse * (scaled - unit * jnp.mean(scaled * unit, axis=-1, keepdims=True))
    ).astype(jnp.bfloat16)
    head_part = transposed_times(logit_cotangent, hidden)
    head_gradient = lax.psum_scatter(
        head_part, "dp", scatter_dimension=0, tiled=True
    )
    pieces = cotangent.reshape(share, replicas, columns_own).transpose(1, 0, 2)
    own_columns, all_tokens = exchange(
        [pieces, token_ids.reshape(1, tokens)], ["swap", "share"], "dp", 3
    )
    (all_columns,) = exchange([own_columns], ["share"], "section", 4)
    cotangent_columns = all_columns.transpose(1, 0, 2, 3).reshape(replicas * tokens, columns_own)
    marks = (all_tokens.reshape(-1, 1) == columns).astype(jnp.bfloat16)
    embed_columns = transposed_times(marks, cotangent_columns)
    (embed_parts,) = exchange(
        [embed_columns.reshape(replicas, slice_rows // replicas, columns_own)], ["swap"], "dp", 5
    )
    embed_gradient = (
        embed_parts.astype(jnp.float32).transpose(1, 0, 2).reshape(slice_rows // replicas, width)
    )
    out_gradient = transposed_times(cotangent_columns, all_mixed)
    out_out = adam_update(out_master, out_first, out_second, out_gradient.reshape(out_master.shape))
    head_out = adam_update(head_master, head_first, head_second, head_gradient)
    embed_out = adam_update(embed_master, embed_first, embed_second, embed_gradient)
    return out_out + head_out + embed_out


def solution(mesh):
    return jax.shard_map(
        local,
        mesh=mesh,
        in_specs=(
            P("section", None, "dp", None),
            P("section", None, "dp", None),
            P(None, "dp"),
            P(None, "dp"),
            P(),
            P("section", None, None),
            P("section", None),
            P("section", "dp", None),
            P("section", "dp", None),
            P("section", "dp", None),
            P(("section", "dp"), None),
            P(("section", "dp"), None),
            P(("section", "dp"), None),
            P(("section", "dp"), None),
            P(("section", "dp"), None),
            P(("section", "dp"), None),
        ),
        out_specs=(
            P("section", "dp", None),
            P("section", "dp", None),
            P("section", "dp", None),
            P(("section", "dp"), None),
            P(("section", "dp"), None),
            P(("section", "dp"), None),
            P(("section", "dp"), None),
            P(("section", "dp"), None),
            P(("section", "dp"), None),
        ),
        check_vma=False,
    )
```

```python
import functools
import jax
import jax.numpy as jnp
from jax import lax
from jax.experimental import pallas as pl
from jax.experimental.pallas import tpu as pltpu
from jax.sharding import PartitionSpec as P

norm_eps = 1e-05
beta_first = 0.9
beta_second = 0.95
adam_eps = 1e-05
learning_rate = 0.0003
decay_rate = 0.1

MESH = pl.DeviceIdType.MESH


def times_transposed(former, latter):
    return lax.dot_general(
        former, latter, (((1,), (1,)), ((), ())), preferred_element_type=jnp.float32
    )


def transposed_times(former, latter):
    return lax.dot_general(
        former, latter, (((0,), (0,)), ((), ())), preferred_element_type=jnp.float32
    )


def plain_times(former, latter):
    return jnp.dot(former, latter, preferred_element_type=jnp.float32)


def adam_update(master, first, second, gradient):
    first_next = beta_first * first + (1.0 - beta_first) * gradient
    second_next = beta_second * second + (1.0 - beta_second) * gradient * gradient
    master_next = master - learning_rate * (
        first_next / (jnp.sqrt(second_next) + adam_eps) + decay_rate * master
    )
    return (master_next, first_next, second_next)


def greet(axis, size, me):
    barrier = pltpu.get_barrier_semaphore()
    for step in range(1, size):
        partner = lax.rem(me + step, size)
        pl.semaphore_signal(barrier, inc=1, device_id={axis: partner}, device_id_type=MESH)
    pl.semaphore_wait(barrier, size - 1)


def exchange_kernel(axis, size, modes, *refs):
    count = len(modes)
    ins, outs = refs[:count], refs[count : 2 * count]
    send_sem, recv_sem = refs[2 * count :]
    me = lax.axis_index(axis)
    greet(axis, size, me)
    copies = []
    for step in range(1, size):
        partner = lax.rem(me + step, size)
        for k, mode in enumerate(modes):
            copy = pltpu.make_async_remote_copy(
                src_ref=ins[k] if mode == "share" else ins[k].at[partner],
                dst_ref=outs[k].at[step - 1 if mode == "others" else me],
                send_sem=send_sem.at[k, step - 1],
                recv_sem=recv_sem.at[k, step - 1],
                device_id={axis: partner},
                device_id_type=MESH,
            )
            copy.start()
            copies.append(copy)
    for k, mode in enumerate(modes):
        if mode != "others":
            outs[k][me] = ins[k][me] if mode == "swap" else ins[k][...]
    for copy in copies:
        copy.wait()


def exchange(arrays, modes, axis, collective_id):
    size = lax.axis_size(axis)
    lead = {"swap": (size,), "share": (size,), "others": (size - 1,)}
    shapes = [
        jax.ShapeDtypeStruct(lead[mode] + (a.shape if mode == "share" else a.shape[1:]), a.dtype)
        for a, mode in zip(arrays, modes)
    ]
    return pl.pallas_call(
        functools.partial(exchange_kernel, axis, size, tuple(modes)),
        out_shape=shapes,
        in_specs=[pl.BlockSpec(memory_space=pltpu.VMEM)] * len(arrays),
        out_specs=[pl.BlockSpec(memory_space=pltpu.VMEM)] * len(arrays),
        scratch_shapes=[
            pltpu.SemaphoreType.DMA((len(arrays), size - 1)),
            pltpu.SemaphoreType.DMA((len(arrays), size - 1)),
        ],
        compiler_params=pltpu.CompilerParams(collective_id=collective_id, has_side_effects=True),
    )(*arrays)


def spread_kernel(axis, size, in_ref, out_ref, send_sem, recv_sem):
    me = lax.axis_index(axis)
    last = size - 1
    second = last // 2
    piece = in_ref.shape[0] // size
    greet(axis, size, me)

    def copy_of(part, target, ref):
        rows = pl.ds(part * piece, piece)
        return pltpu.make_async_remote_copy(
            src_ref=ref.at[rows],
            dst_ref=out_ref.at[rows],
            send_sem=send_sem.at[part, target],
            recv_sem=recv_sem.at[part],
            device_id={axis: target},
            device_id_type=MESH,
        )

    def relayed(device):
        return [device, last] if device == second else [device]

    @pl.when(me == last)
    def _():
        copies = [copy_of(part, k, in_ref) for k in range(last) for part in relayed(k)]
        for copy in copies:
            copy.start()
        out_ref[...] = in_ref[...]
        for copy in copies:
            copy.wait_send()

    for device in range(last):

        @pl.when(me == device)
        def _():
            others = [k for k in range(last) if k != device]
            copies = []
            for part in relayed(device):
                copy_of(part, others[0], out_ref).wait_recv()
                for k in others:
                    copies.append(copy_of(part, k, out_ref))
                    copies[-1].start()
            for part in range(size):
                if part not in relayed(device):
                    copy_of(part, others[0], out_ref).wait_recv()
            for copy in copies:
                copy.wait_send()


def spread(block, axis, collective_id):
    size = lax.axis_size(axis)
    return pl.pallas_call(
        functools.partial(spread_kernel, axis, size),
        out_shape=jax.ShapeDtypeStruct(block.shape, block.dtype),
        in_specs=[pl.BlockSpec(memory_space=pltpu.VMEM)],
        out_specs=pl.BlockSpec(memory_space=pltpu.VMEM),
        scratch_shapes=[
            pltpu.SemaphoreType.DMA((size, size)),
            pltpu.SemaphoreType.DMA((size,)),
        ],
        compiler_params=pltpu.CompilerParams(collective_id=collective_id, has_side_effects=True),
        name="spread",
    )(block)


def local(
    block_inputs,
    mixed_inputs,
    token_ids,
    target_ids,
    final_gain,
    out_weight,
    head_weight,
    out_master,
    out_first,
    out_second,
    head_master,
    head_first,
    head_second,
    embed_master,
    embed_first,
    embed_second,
):
    sections = lax.axis_size("section")
    replicas = lax.axis_size("dp")
    section = lax.axis_index("section")
    last = sections - 1
    batches, rows, width = mixed_inputs[0].shape
    tokens = batches * rows
    share = tokens // sections
    columns_own = width // replicas
    flat_mixed = mixed_inputs[0].reshape(tokens, width)
    all_mixed = lax.all_gather(flat_mixed, "dp", tiled=True)
    wide = block_inputs[0].reshape(tokens, width).astype(jnp.float32)
    slice_rows = head_weight.shape[0]
    vocabulary_start = section * slice_rows
    columns = vocabulary_start + lax.broadcasted_iota(jnp.int32, (1, slice_rows), 1)
    final = wide + times_transposed(flat_mixed, out_weight[0])
    final_inverse = lax.rsqrt(jnp.mean(final * final, axis=-1, keepdims=True) + norm_eps)
    own_hidden = (final * final_inverse * final_gain).astype(jnp.bfloat16)
    hidden = spread(own_hidden, "section", 0)
    logits = times_transposed(hidden, head_weight)
    local_top = jnp.max(logits, axis=1)
    local_weights = jnp.exp(logits - local_top[:, None])
    (stats,) = exchange(
        [jnp.stack([local_top, jnp.sum(local_weights, axis=1), final_inverse[:, 0]])],
        ["share"],
        "section",
        1,
    )
    row_top = jnp.max(stats[:, 0], axis=0)
    row_total = jnp.sum(stats[:, 1] * jnp.exp(stats[:, 0] - row_top), axis=0)
    predicted = local_weights * (jnp.exp(local_top - row_top) / row_total)[:, None]
    target_flat = target_ids.reshape(-1)
    logit_cotangent = jnp.where(target_flat[:, None] == columns, predicted - 1.0, predicted).astype(
        jnp.bfloat16
    )
    hidden_part = plain_times(logit_cotangent, head_weight).reshape(sections, share, width)
    (hidden_parts,) = exchange(
        [hidden_part], ["others"], "section", 2
    )
    hidden_cotangent = (
        lax.dynamic_index_in_dim(hidden_part, section, 0, False)
        + jnp.sum(hidden_parts, axis=0)
    )
    inverse = lax.dynamic_slice_in_dim(stats[last, 2], section * share, share)[:, None]
    unit = lax.dynamic_slice_in_dim(hidden, section * share, share).astype(jnp.float32) / final_gain
    scaled = hidden_cotangent * final_gain
    cotangent = (
        inverse * (scaled - unit * jnp.mean(scaled * unit, axis=-1, keepdims=True))
    ).astype(jnp.bfloat16)
    head_part = transposed_times(logit_cotangent, hidden)
    head_gradient = lax.psum_scatter(
        head_part, "dp", scatter_dimension=0, tiled=True
    )
    pieces = cotangent.reshape(share, replicas, columns_own).transpose(1, 0, 2)
    own_columns, all_tokens = exchange(
        [pieces, token_ids.reshape(1, tokens)], ["swap", "share"], "dp", 3
    )
    (all_columns,) = exchange([own_columns], ["share"], "section", 4)
    cotangent_columns = all_columns.transpose(1, 0, 2, 3).reshape(replicas * tokens, columns_own)
    marks = (all_tokens.reshape(-1, 1) == columns).astype(jnp.bfloat16)
    embed_columns = transposed_times(marks, cotangent_columns)
    embed_blocks = embed_columns.reshape(replicas, slice_rows // replicas, columns_own)
    replica = lax.axis_index("dp")
    embed_steps = []
    for step in range(replicas):
        block = lax.dynamic_index_in_dim(embed_blocks, (replica + step) % replicas, 0, False)
        route = [(i, (i + step) % replicas) for i in range(replicas)]
        embed_steps.append(lax.ppermute(block, "dp", route) if step else block)
    embed_parts = jnp.roll(jnp.stack(embed_steps[::-1]), replica + 1, axis=0)
    embed_gradient = (
        embed_parts.astype(jnp.float32).transpose(1, 0, 2).reshape(slice_rows // replicas, width)
    )
    out_gradient = transposed_times(cotangent_columns, all_mixed)
    out_out = adam_update(out_master, out_first, out_second, out_gradient.reshape(out_master.shape))
    head_out = adam_update(head_master, head_first, head_second, head_gradient)
    embed_out = adam_update(embed_master, embed_first, embed_second, embed_gradient)
    return out_out + head_out + embed_out


def solution(mesh):
    return jax.shard_map(
        local,
        mesh=mesh,
        in_specs=(
            P("section", None, "dp", None),
            P("section", None, "dp", None),
            P(None, "dp"),
            P(None, "dp"),
            P(),
            P("section", None, None),
            P("section", None),
            P("section", "dp", None),
            P("section", "dp", None),
            P("section", "dp", None),
            P(("section", "dp"), None),
            P(("section", "dp"), None),
            P(("section", "dp"), None),
            P(("section", "dp"), None),
            P(("section", "dp"), None),
            P(("section", "dp"), None),
        ),
        out_specs=(
            P("section", "dp", None),
            P("section", "dp", None),
            P("section", "dp", None),
            P(("section", "dp"), None),
            P(("section", "dp"), None),
            P(("section", "dp"), None),
            P(("section", "dp"), None),
            P(("section", "dp"), None),
            P(("section", "dp"), None),
        ),
        check_vma=False,
    )
```
